32 devices in a mesh: section: 2 (over y), seq: 4 (over z), tp: 4 (over x, core).
Axes of the slice: x: 2, y: 2, z: 4, core: 2. Of those that a mesh axis runs over, the one named last changes fastest.
Arguments:
- layer_input: bfloat16 [2, 1024, 4096], P('section', 'seq'), may hold values from -500 to 500
- upstream: bfloat16 [2, 1024, 4096], P('section', 'seq'), may hold values from -6 to 6
- norm_gain: bfloat16 [2, 4096], P('section'), may hold values from 0.5 to 1.5
- query_weight: bfloat16 [2, 4096, 2048], P('section', 'seq', 'tp'), may hold values from -0.0625 to 0.0625
- key_weight: bfloat16 [2, 4096, 1024], P('section', 'seq', 'tp'), may hold values from -0.0625 to 0.0625
- value_weight: bfloat16 [2, 4096, 1024], P('section', 'seq', 'tp'), may hold values from -0.09375 to 0.09375
- output_weight: bfloat16 [2, 4096, 2048], P('section', 'seq', 'tp'), may hold values from -0.125 to 0.125
Outputs:
- passed_grad: bfloat16 [2, 1024, 4096], P('section', 'seq')
- query_grad: bfloat16 [2, 4096, 2048], P('section', 'seq', 'tp')
- key_grad: bfloat16 [2, 4096, 1024], P('section', 'seq', 'tp')
- value_grad: bfloat16 [2, 4096, 1024], P('section', 'seq', 'tp')
- output_grad: bfloat16 [2, 4096, 2048], P('section', 'seq', 'tp')
- gain_grad: float32 [2, 4096], P('section', 'tp')
The draws below stay inside these ranges and needn't reach their ends.
All inputs are finite; a program needn't handle non-finite values.
Results may differ from the reference program's by a relative error of at most 0.023.
Values may be sent and summed in bfloat16 or wider, within the bound.
No kernel may reach another device: no remote copies, remote signals or barrier semaphores. Data moves between devices by JAX's collectives and lax.ppermute only.
A program may use at most 128 MiB of HBM per device.

```python
import math
import jax
import jax.numpy as jnp
from jax import lax

D = 4096
HEADS = 16
KV_HEADS = 8
HEAD_DIM = 128
WINDOW = 2048
BLOCK = 256
TOKENS = 1024
N_SEQ = 4
N_TP = 4


def projection_pair(base_key):
    fan_scale = 1.0 / math.sqrt(D)
    query_part = jnp.clip(jax.random.normal(jax.random.fold_in(base_key, 101), (2, D, HEADS * HEAD_DIM), jnp.float32), -4.0, 4.0) * fan_scale
    key_part = jnp.clip(jax.random.normal(jax.random.fold_in(base_key, 102), (2, D, KV_HEADS * HEAD_DIM), jnp.float32), -4.0, 4.0) * fan_scale
    return (query_part, key_part)


def draw_query_weight(key, part):
    return projection_pair(key)[0].astype(jnp.bfloat16)


def draw_key_weight(key, part):
    return projection_pair(key)[1].astype(jnp.bfloat16)


def draw_layer_input(key, part):
    noise_field = jnp.clip(jax.random.normal(jax.random.fold_in(key, 103), (2, TOKENS, D), jnp.float32), -6.0, 6.0)
    return noise_field.astype(jnp.bfloat16)


def steps_of(own_key, dims, pieces, smallest, top_value):
    level = 1.0
    for axis_at, blocks in pieces:
        draws = jax.random.uniform(jax.random.fold_in(jax.random.fold_in(own_key, 6), axis_at), (blocks,), jnp.float32, smallest / len(pieces), top_value / len(pieces))
        level = level * jnp.repeat(jnp.exp(draws), dims[axis_at] // blocks).reshape((-1,) + (1,) * (len(dims) - 1 - axis_at))
    return level


def noise(rng, extent, deviation, bound, split=(), kind=jnp.bfloat16):
    loudness = steps_of(rng, extent, split, -0.22, 0.18) if split else 1.0
    drawn = jax.random.normal(rng, extent, jnp.float32) * deviation * loudness
    return jnp.minimum(jnp.maximum(drawn, -bound), bound).astype(kind)


def setup_inputs(seed: int = 0) -> dict:
    key_of = jax.random.split(jax.random.key(seed), 8)
    return {
        "layer_input": draw_layer_input(jax.random.fold_in(key_of[7], 71), 0),
        "upstream": noise(key_of[1], (2, TOKENS, D), 1.0, 6.0, ((0, 2), (1, 4))),
        "norm_gain": jnp.clip(1.0 + 0.1 * jax.random.normal(key_of[2], (2, D), jnp.float32), 0.5, 1.5).astype(jnp.bfloat16),
        "query_weight": draw_query_weight(jax.random.fold_in(key_of[7], 71), 0),
        "key_weight": draw_key_weight(jax.random.fold_in(key_of[7], 71), 0),
        "value_weight": noise(key_of[5], (2, D, KV_HEADS * HEAD_DIM), D ** -0.5, 0.09375, ((0, 2), (1, 4), (2, 4))),
        "output_weight": noise(key_of[6], (2, D, HEADS * HEAD_DIM), (HEADS * HEAD_DIM) ** -0.5, 0.125, ((0, 2), (1, 4), (2, 4))),
    }


epsilon = 1e-05

def rotate(values, positions, direction_sign):
    half_width = values.shape[-1] // 2
    frequency = jnp.exp(jnp.arange(half_width, dtype=jnp.float32) * (-2.0 * math.log(10000.0) / values.shape[-1]))
    angles = positions[:, None] * frequency[None, :]
    cosine = jnp.cos(angles)[:, None, :]
    sine_table = direction_sign * jnp.sin(angles)[:, None, :]
    first_half = values[..., :half_width]
    second_half = values[..., half_width:]
    return jnp.concatenate([first_half * cosine - second_half * sine_table, second_half * cosine + first_half * sine_table], axis=-1)

def layer_backward(layer_input, upstream, norm_gain, query_weight, key_weight, value_weight, output_weight):
    tokens_all = layer_input.shape[0]
    input_values = layer_input.astype(jnp.float32)
    inverse_norm = lax.rsqrt(lax.optimization_barrier(jnp.mean(input_values * input_values, axis=-1, keepdims=True)) + epsilon)
    gain_values = norm_gain.astype(jnp.float32)
    normed = (input_values * inverse_norm * gain_values).astype(jnp.bfloat16)
    positions = jnp.arange(tokens_all).astype(jnp.float32)
    query_vectors = rotate(jnp.dot(normed, query_weight, preferred_element_type=jnp.float32).reshape(tokens_all, HEADS, HEAD_DIM), positions, 1.0).astype(jnp.bfloat16)
    key_vectors = rotate(jnp.dot(normed, key_weight, preferred_element_type=jnp.float32).reshape(tokens_all, KV_HEADS, HEAD_DIM), positions, 1.0).astype(jnp.bfloat16)
    value_vectors = jnp.dot(normed, value_weight, preferred_element_type=jnp.float32).astype(jnp.bfloat16).reshape(tokens_all, KV_HEADS, HEAD_DIM)
    attn_delta = jnp.dot(upstream, output_weight, preferred_element_type=jnp.float32).astype(jnp.bfloat16).reshape(tokens_all, HEADS, HEAD_DIM)
    group_size = HEADS // KV_HEADS
    score_scale = 1.0 / math.sqrt(HEAD_DIM)
    halo_blocks = min((WINDOW + BLOCK - 2) // BLOCK, N_SEQ - 1)
    span_rows = (halo_blocks + 1) * BLOCK
    pad_rows = halo_blocks * BLOCK
    padding = jnp.zeros((pad_rows, KV_HEADS, HEAD_DIM), jnp.bfloat16)
    keys_padded = jnp.concatenate([padding, key_vectors], axis=0)
    values_padded = jnp.concatenate([padding, value_vectors], axis=0)

    def attend(carry, block_index):
        key_total, value_total = carry
        first_row = (block_index * BLOCK).astype(jnp.int32)
        query_block = lax.dynamic_slice_in_dim(query_vectors, first_row, BLOCK, 0).astype(jnp.float32)
        delta_block = lax.dynamic_slice_in_dim(attn_delta, first_row, BLOCK, 0).astype(jnp.float32)
        key_slab = lax.dynamic_slice_in_dim(keys_padded, first_row, span_rows, 0).astype(jnp.float32)
        value_slab = lax.dynamic_slice_in_dim(values_padded, first_row, span_rows, 0).astype(jnp.float32)
        key_heads = jnp.repeat(key_slab, group_size, axis=1)
        value_heads = jnp.repeat(value_slab, group_size, axis=1)
        query_position = first_row + jnp.arange(BLOCK).astype(jnp.int32)
        key_position = first_row - pad_rows + jnp.arange(span_rows).astype(jnp.int32)
        allowed = (key_position[None, :] <= query_position[:, None]) & (key_position[None, :] > query_position[:, None] - WINDOW) & (key_position[None, :] >= 0)
        scores = jnp.einsum('thd,uhd->htu', query_block, key_heads) * score_scale
        scores = jnp.where(allowed[None], scores, -1e+30)
        row_peak = lax.optimization_barrier(jnp.max(scores, axis=-1, keepdims=True))
        exponent_terms = jnp.exp(scores - row_peak)
        softmax_probs = exponent_terms / lax.optimization_barrier(jnp.sum(exponent_terms, axis=-1, keepdims=True))
        rounded_probs = softmax_probs.astype(jnp.bfloat16).astype(jnp.float32)
        attended = jnp.einsum('htu,uhd->thd', rounded_probs, value_heads).astype(jnp.bfloat16)
        softmax_delta = jnp.einsum('thd,uhd->htu', delta_block, value_heads)
        row_delta = lax.optimization_barrier(jnp.sum(delta_block * attended.astype(jnp.float32), axis=-1))
        score_delta = (softmax_probs * (softmax_delta - jnp.transpose(row_delta)[:, :, None]) * score_scale).astype(jnp.bfloat16).astype(jnp.float32)
        query_rot_delta = jnp.einsum('htu,uhd->thd', score_delta, key_heads)
        key_part = jnp.einsum('htu,thd->uhd', score_delta, query_block).reshape(span_rows, KV_HEADS, group_size, HEAD_DIM).sum(axis=2)
        value_part = jnp.einsum('htu,thd->uhd', rounded_probs, delta_block).reshape(span_rows, KV_HEADS, group_size, HEAD_DIM).sum(axis=2)
        key_total = lax.dynamic_update_slice_in_dim(key_total, lax.dynamic_slice_in_dim(key_total, first_row, span_rows, 0) + key_part, first_row, 0)
        value_total = lax.dynamic_update_slice_in_dim(value_total, lax.dynamic_slice_in_dim(value_total, first_row, span_rows, 0) + value_part, first_row, 0)
        return ((key_total, value_total), (attended, query_rot_delta))
    start_carry = (jnp.zeros((pad_rows + tokens_all, KV_HEADS, HEAD_DIM), jnp.float32), jnp.zeros((pad_rows + tokens_all, KV_HEADS, HEAD_DIM), jnp.float32))
    (key_total, value_total), (attended, query_rot_delta) = lax.scan(attend, start_carry, jnp.arange(N_SEQ).astype(jnp.int32))
    attended = attended.reshape(tokens_all, HEADS * HEAD_DIM)
    query_rot_delta = query_rot_delta.reshape(tokens_all, HEADS, HEAD_DIM)
    query_delta = rotate(query_rot_delta, positions, -1.0).astype(jnp.bfloat16).reshape(tokens_all, HEADS * HEAD_DIM)
    key_delta = rotate(key_total[pad_rows:], positions, -1.0).astype(jnp.bfloat16).reshape(tokens_all, KV_HEADS * HEAD_DIM)
    value_delta = value_total[pad_rows:].astype(jnp.bfloat16).reshape(tokens_all, KV_HEADS * HEAD_DIM)
    head_share = HEADS // N_TP * HEAD_DIM
    kv_share = KV_HEADS // N_TP * HEAD_DIM
    normed_delta = jnp.zeros((tokens_all, D), jnp.float32)
    for group_index in range(N_TP):
        query_cols = slice(group_index * head_share, (group_index + 1) * head_share)
        kv_cols = slice(group_index * kv_share, (group_index + 1) * kv_share)
        partial_value = jnp.dot(query_delta[:, query_cols], query_weight[:, query_cols].T, preferred_element_type=jnp.float32)
        partial_value = partial_value + jnp.dot(key_delta[:, kv_cols], key_weight[:, kv_cols].T, preferred_element_type=jnp.float32)
        partial_value = partial_value + jnp.dot(value_delta[:, kv_cols], value_weight[:, kv_cols].T, preferred_element_type=jnp.float32)
        normed_delta = normed_delta + lax.optimization_barrier(partial_value.astype(jnp.bfloat16)).astype(jnp.float32)
    row_dot = lax.optimization_barrier(jnp.sum(gain_values * normed_delta * input_values, axis=-1, keepdims=True))
    input_delta = (upstream.astype(jnp.float32) + inverse_norm * gain_values * normed_delta - input_values * inverse_norm * inverse_norm * inverse_norm * row_dot / D).astype(jnp.bfloat16)
    gain_grad = lax.optimization_barrier(jnp.sum(normed_delta * input_values * inverse_norm, axis=0))
    deltas_all = jnp.concatenate([query_delta, key_delta, value_delta], axis=1)

    def seq_partial(totals, block_index):
        first_row = (block_index * BLOCK).astype(jnp.int32)
        normed_rows = lax.dynamic_slice_in_dim(normed, first_row, BLOCK, 0)
        delta_rows = lax.dynamic_slice_in_dim(deltas_all, first_row, BLOCK, 0)
        upstream_rows = lax.dynamic_slice_in_dim(upstream, first_row, BLOCK, 0)
        attended_rows = lax.dynamic_slice_in_dim(attended, first_row, BLOCK, 0)
        part_in = jnp.dot(normed_rows.T, delta_rows, preferred_element_type=jnp.float32)
        part_out = jnp.dot(upstream_rows.T, attended_rows, preferred_element_type=jnp.float32)
        part_in = lax.optimization_barrier(part_in.astype(jnp.bfloat16)).astype(jnp.float32)
        part_out = lax.optimization_barrier(part_out.astype(jnp.bfloat16)).astype(jnp.float32)
        return ((totals[0] + part_in, totals[1] + part_out), None)
    zero_in = jnp.zeros((D, (HEADS + 2 * KV_HEADS) * HEAD_DIM), jnp.float32)
    zero_out = jnp.zeros((D, HEADS * HEAD_DIM), jnp.float32)
    (grads_in, grads_out), unused = lax.scan(seq_partial, (zero_in, zero_out), jnp.arange(N_SEQ).astype(jnp.int32))
    query_grad = grads_in[:, :HEADS * HEAD_DIM].astype(jnp.bfloat16)
    key_grad = grads_in[:, HEADS * HEAD_DIM:(HEADS + KV_HEADS) * HEAD_DIM].astype(jnp.bfloat16)
    value_grad = grads_in[:, (HEADS + KV_HEADS) * HEAD_DIM:].astype(jnp.bfloat16)
    output_grad = grads_out.astype(jnp.bfloat16)
    return (input_delta, query_grad, key_grad, value_grad, output_grad, gain_grad)

def reference(layer_input, upstream, norm_gain, query_weight, key_weight, value_weight, output_weight):
    results = []
    for section_index in range(2):
        results.append(layer_backward(layer_input[section_index], upstream[section_index], norm_gain[section_index], query_weight[section_index], key_weight[section_index], value_weight[section_index], output_weight[section_index]))
    passed_grad = jnp.stack([results[1][0], results[0][0]], axis=0)
    query_grad = jnp.stack([results[0][1], results[1][1]], axis=0)
    key_grad = jnp.stack([results[0][2], results[1][2]], axis=0)
    value_grad = jnp.stack([results[0][3], results[1][3]], axis=0)
    output_grad = jnp.stack([results[0][4], results[1][4]], axis=0)
    gain_grad = jnp.stack([results[0][5], results[1][5]], axis=0)
    return (passed_grad, query_grad, key_grad, value_grad, output_grad, gain_grad)
```

```python
import math

import jax
import jax.numpy as jnp
from jax import lax
from jax.experimental import pallas as pl
from jax.experimental.pallas import tpu as pltpu
from jax.sharding import PartitionSpec as P

HEAD_DIM = 128
WINDOW = 2048
BLOCK_ROWS = 256


epsilon = 1e-05


def shifted(value, axis, steps):
    count = lax.axis_size(axis)
    leading, last = (max(0, -steps), min(count, count - steps))
    return lax.ppermute(value, axis, [(source, source + steps) for source in range(leading, last)])


def shifted_2(value, axis, steps):
    count = lax.axis_size(axis)
    pairs = [(source, (source + steps) % count) for source in range(count)]
    return lax.ppermute(value, axis, pairs)


def rotate(values, positions, direction_sign):
    half_width = values.shape[-1] // 2
    frequency = jnp.exp(
        jnp.arange(half_width, dtype=jnp.float32) * (-2.0 * math.log(10000.0) / values.shape[-1])
    )
    angles = positions[:, None] * frequency[None, :]
    cosine = jnp.cos(angles)[:, None, :]
    sine_table = direction_sign * jnp.sin(angles)[:, None, :]
    first_half = values[..., :half_width]
    second_half = values[..., half_width:]
    return jnp.concatenate(
        [
            first_half * cosine - second_half * sine_table,
            second_half * cosine + first_half * sine_table,
        ],
        axis=-1,
    )


def contract_rows(left_side, right_side):
    return lax.dot_general(
        left_side, right_side, (((0,), (0,)), ((), ())), preferred_element_type=jnp.float32
    )


def contract_last(left_side, right_side):
    return lax.dot_general(
        left_side, right_side, (((1,), (1,)), ((), ())), preferred_element_type=jnp.float32
    )


def per_device_rows(
    layer_input, upstream, norm_gain, query_weight, key_weight, value_weight, output_weight
):
    input_rows = layer_input[0]
    upstream_rows = upstream[0]
    block_rows = input_rows.shape[0]
    model_width = input_rows.shape[1]
    seq_count = lax.axis_size("seq")
    seq_index = lax.axis_index("seq")
    tp_count = lax.axis_size("tp")
    tp_index = lax.axis_index("tp")
    query_cols = query_weight.shape[2]
    kv_cols = key_weight.shape[2]
    local_heads = query_cols // HEAD_DIM
    local_groups = kv_cols // HEAD_DIM
    group_size = local_heads // local_groups
    halo_blocks = min((WINDOW + block_rows - 2) // block_rows, seq_count - 1)
    span_rows = (halo_blocks + 1) * block_rows
    score_scale = 1.0 / math.sqrt(HEAD_DIM)
    share_width = model_width // tp_count
    input_values = input_rows.astype(jnp.float32)
    inverse_norm = lax.rsqrt(
        jnp.mean(input_values * input_values, axis=-1, keepdims=True) + epsilon
    )
    gain_values = norm_gain[0].astype(jnp.float32)
    normed = (input_values * inverse_norm * gain_values).astype(jnp.bfloat16)
    gathered = (
        lax.all_gather(query_weight, "seq", axis=1, tiled=True),
        lax.all_gather(key_weight, "seq", axis=1, tiled=True),
        lax.all_gather(value_weight, "seq", axis=1, tiled=True),
        lax.all_gather(output_weight, "seq", axis=1, tiled=True),
    )
    query_full = gathered[0][0]
    key_full = gathered[1][0]
    value_full = gathered[2][0]
    output_full = gathered[3][0]
    first_position = seq_index * block_rows
    positions = (first_position + jnp.arange(block_rows)).astype(jnp.float32)
    query_vectors = rotate(
        jnp.dot(normed, query_full, preferred_element_type=jnp.float32).reshape(
            block_rows, local_heads, HEAD_DIM
        ),
        positions,
        1.0,
    ).astype(jnp.bfloat16)
    key_vectors = rotate(
        jnp.dot(normed, key_full, preferred_element_type=jnp.float32).reshape(
            block_rows, local_groups, HEAD_DIM
        ),
        positions,
        1.0,
    ).astype(jnp.bfloat16)
    value_vectors = (
        jnp.dot(normed, value_full, preferred_element_type=jnp.float32)
        .astype(jnp.bfloat16)
        .reshape(block_rows, local_groups, HEAD_DIM)
    )
    attn_delta = (
        jnp.dot(upstream_rows, output_full, preferred_element_type=jnp.float32)
        .astype(jnp.bfloat16)
        .reshape(block_rows, local_heads, HEAD_DIM)
    )
    everything = (
        lax.all_gather(key_vectors, "seq", axis=0, tiled=True),
        lax.all_gather(value_vectors, "seq", axis=0, tiled=True),
    )
    padding = jnp.zeros((halo_blocks * block_rows, local_groups, HEAD_DIM), jnp.bfloat16)
    key_slab = lax.dynamic_slice_in_dim(
        jnp.concatenate([padding, everything[0]], axis=0), first_position, span_rows, 0
    )
    value_slab = lax.dynamic_slice_in_dim(
        jnp.concatenate([padding, everything[1]], axis=0), first_position, span_rows, 0
    )
    query_position = first_position + jnp.arange(block_rows)
    key_position = (seq_index - halo_blocks) * block_rows + jnp.arange(span_rows)
    allowed = (
        (key_position[None, :] <= query_position[:, None])
        & (key_position[None, :] > query_position[:, None] - WINDOW)
        & (key_position[None, :] >= 0)
    )
    attended_parts = []
    query_grad_parts = []
    key_accum = [
        jnp.zeros((span_rows, HEAD_DIM), jnp.float32) for group_index in range(local_groups)
    ]
    value_accum = [
        jnp.zeros((span_rows, HEAD_DIM), jnp.float32) for group_index in range(local_groups)
    ]
    for head_index in range(local_heads):
        group_index = head_index // group_size
        query_head = query_vectors[:, head_index, :]
        keys_head = key_slab[:, group_index, :]
        values_head = value_slab[:, group_index, :]
        delta_head = attn_delta[:, head_index, :]
        scores = jnp.where(allowed, contract_last(query_head, keys_head) * score_scale, -1e30)
        row_peak = jnp.max(scores, axis=-1, keepdims=True)
        exponent_terms = jnp.exp(scores - row_peak)
        softmax_probs = exponent_terms / jnp.sum(exponent_terms, axis=-1, keepdims=True)
        rounded_probs = softmax_probs.astype(jnp.bfloat16)
        attended_head = jnp.dot(
            rounded_probs, values_head, preferred_element_type=jnp.float32
        ).astype(jnp.bfloat16)
        softmax_delta = contract_last(delta_head, values_head)
        row_delta = jnp.sum(
            delta_head.astype(jnp.float32) * attended_head.astype(jnp.float32),
            axis=-1,
            keepdims=True,
        )
        score_delta = (softmax_probs * (softmax_delta - row_delta) * score_scale).astype(
            jnp.bfloat16
        )
        query_grad_parts.append(jnp.dot(score_delta, keys_head, preferred_element_type=jnp.float32))
        key_accum[group_index] = key_accum[group_index] + contract_rows(score_delta, query_head)
        value_accum[group_index] = value_accum[group_index] + contract_rows(
            rounded_probs, delta_head
        )
        attended_parts.append(attended_head)
    key_slab_grad = jnp.stack(key_accum, axis=1)
    value_slab_grad = jnp.stack(value_accum, axis=1)
    key_total = key_slab_grad[halo_blocks * block_rows :]
    value_total = value_slab_grad[halo_blocks * block_rows :]
    for distance in range(1, halo_blocks + 1):
        first_row = (halo_blocks - distance) * block_rows
        arrived = (
            shifted(
                key_slab_grad[first_row : first_row + block_rows].astype(jnp.bfloat16),
                "seq",
                -distance,
            ).astype(jnp.float32),
            shifted(
                value_slab_grad[first_row : first_row + block_rows].astype(jnp.bfloat16),
                "seq",
                -distance,
            ).astype(jnp.float32),
        )
        key_total = key_total + arrived[0]
        value_total = value_total + arrived[1]
    query_delta = (
        rotate(jnp.stack(query_grad_parts, axis=1), positions, -1.0)
        .astype(jnp.bfloat16)
        .reshape(block_rows, query_cols)
    )
    key_delta = rotate(key_total, positions, -1.0).astype(jnp.bfloat16).reshape(block_rows, kv_cols)
    value_delta = value_total.astype(jnp.bfloat16).reshape(block_rows, kv_cols)
    attended_flat = jnp.stack(attended_parts, axis=1).reshape(block_rows, query_cols)
    normed_partial = (
        contract_last(query_delta, query_full)
        + contract_last(key_delta, key_full)
        + contract_last(value_delta, value_full)
    )
    share_start = tp_index * share_width
    input_share = lax.dynamic_slice_in_dim(input_values, share_start, share_width, 1)
    cube_norm = inverse_norm * inverse_norm * inverse_norm
    normed_delta = lax.psum(normed_partial.astype(jnp.bfloat16), "tp").astype(jnp.float32)
    row_dot = jnp.sum(gain_values * normed_delta * input_values, axis=-1, keepdims=True)
    input_delta = (
        upstream_rows.astype(jnp.float32)
        + inverse_norm * gain_values * normed_delta
        - input_values * cube_norm * row_dot / model_width
    ).astype(jnp.bfloat16)
    delta_share = lax.dynamic_slice_in_dim(normed_delta, share_start, share_width, 1)
    gain_part = jnp.sum(delta_share * input_share * inverse_norm, axis=0)
    gain_total = lax.psum(gain_part, "seq")
    passed = shifted_2(input_delta[None], "section", -1)
    deltas_all = jnp.concatenate([query_delta, key_delta, value_delta], axis=1)
    summed_grads = lax.psum_scatter(
        jnp.concatenate(
            [contract_rows(normed, deltas_all), contract_rows(upstream_rows, attended_flat)], axis=1
        ).astype(jnp.bfloat16),
        "seq",
        scatter_dimension=0,
        tiled=True,
    )
    query_grad = summed_grads[:, :query_cols]
    key_grad = summed_grads[:, query_cols : query_cols + kv_cols]
    value_grad = summed_grads[:, query_cols + kv_cols : query_cols + 2 * kv_cols]
    output_grad = summed_grads[:, query_cols + 2 * kv_cols :]
    return (
        passed,
        query_grad[None],
        key_grad[None],
        value_grad[None],
        output_grad[None],
        gain_total[None],
    )


def turn(value, axis, steps):
    count = lax.axis_size(axis)
    return lax.ppermute(value, axis, [(source, (source + steps) % count) for source in range(count)])


def swap(value, axis, bit):
    count = lax.axis_size(axis)
    return lax.ppermute(value, axis, [(source, source ^ bit) for source in range(count)])


def columns(value, start, width):
    return lax.dynamic_slice_in_dim(value, start, width, value.ndim - 1)


def half_swapped(values):
    half_width = values.shape[-1] // 2
    return jnp.concatenate([values[..., half_width:], values[..., :half_width]], axis=-1)


def rotary_tables(count):
    half_width = HEAD_DIM // 2
    frequency = jnp.exp(
        jnp.arange(half_width, dtype=jnp.float32) * (-2.0 * math.log(10000.0) / HEAD_DIM)
    )
    angles = jnp.arange(count).astype(jnp.float32)[:, None] * frequency[None, :]
    cosine = jnp.cos(angles)
    sine = jnp.sin(angles)
    return jnp.concatenate([cosine, cosine], axis=1), jnp.concatenate([-sine, sine], axis=1)


def attention_kernel(
    query_ref,
    key_ref,
    value_ref,
    delta_ref,
    cosine_ref,
    sine_ref,
    query_out,
    attended_out,
    key_out,
    value_out,
    key_sum,
    value_sum,
):
    total = query_ref.shape[0]
    block = min(BLOCK_ROWS, total)
    scale = 1.0 / math.sqrt(HEAD_DIM)

    def unrotated(values, first, count):
        cosine = cosine_ref[first : first + count, :]
        sine = sine_ref[first : first + count, :]
        return values * cosine - pltpu.roll(values, HEAD_DIM // 2, 1) * sine

    key_sum[...] = jnp.zeros_like(key_sum)
    value_sum[...] = jnp.zeros_like(value_sum)
    for first in range(0, total, block):
        span = first + block
        query = query_ref[first:span, :]
        delta = delta_ref[first:span, :]
        keys = key_ref[:span, :]
        values = value_ref[:span, :]
        scores = contract_last(query, keys) * scale
        row = lax.broadcasted_iota(jnp.int32, scores.shape, 0) + first
        column = lax.broadcasted_iota(jnp.int32, scores.shape, 1)
        scores = jnp.where(column <= row, scores, -1e30)
        terms = jnp.exp(scores - jnp.max(scores, axis=-1, keepdims=True))
        probs = terms / jnp.sum(terms, axis=-1, keepdims=True)
        rounded = probs.astype(jnp.bfloat16)
        attended = jnp.dot(rounded, values, preferred_element_type=jnp.float32).astype(jnp.bfloat16)
        attended_out[first:span, :] = attended
        row_delta = jnp.sum(
            delta.astype(jnp.float32) * attended.astype(jnp.float32), axis=-1, keepdims=True
        )
        score_delta = (probs * (contract_last(delta, values) - row_delta) * scale).astype(
            jnp.bfloat16
        )
        query_turned = jnp.dot(score_delta, keys, preferred_element_type=jnp.float32)
        query_out[first:span, :] = unrotated(query_turned, first, block).astype(jnp.bfloat16)
        key_sum[:span, :] += contract_rows(score_delta, query)
        value_sum[:span, :] += contract_rows(rounded, delta)
    key_out[...] = unrotated(key_sum[...], 0, total).astype(jnp.bfloat16)
    value_out[...] = value_sum[...].astype(jnp.bfloat16)


def attend(query, key, value, delta, cosine, sine):
    shape = jax.ShapeDtypeStruct(query.shape, jnp.bfloat16)
    return pl.pallas_call(
        attention_kernel,
        out_shape=(shape,) * 4,
        scratch_shapes=[pltpu.VMEM(query.shape, jnp.float32)] * 2,
        compiler_params=pltpu.CompilerParams(vmem_limit_bytes=48 * 1024 * 1024),
        name="attend",
    )(query, key, value, delta, cosine, sine)


def gathered_line(value, axis):
    count = lax.axis_size(axis)
    index = lax.axis_index(axis)
    rights, lefts = [value], [value]
    for step in range(1, count):
        rights.append(shifted(rights[-1], axis, 1))
        lefts.append(shifted(lefts[-1], axis, -1))
    found = [value]
    for ahead in range(1, count):
        found.append(jnp.where(index + ahead < count, lefts[ahead], rights[count - ahead]))
    return found


def per_device_heads(
    layer_input, upstream, norm_gain, query_weight, key_weight, value_weight, output_weight
):
    input_rows = layer_input[0]
    upstream_rows = upstream[0]
    block_rows, model_width = input_rows.shape
    seq_count = lax.axis_size("seq")
    seq_index = lax.axis_index("seq")
    tp_count = lax.axis_size("tp")
    tp_index = lax.axis_index("tp")
    query_block = query_weight[0]
    key_block = key_weight[0]
    value_block = value_weight[0]
    output_block = output_weight[0]
    local_width = query_block.shape[0]
    local_heads = query_block.shape[1] // HEAD_DIM
    local_groups = key_block.shape[1] // HEAD_DIM
    total_rows = seq_count * block_rows
    half_rows = block_rows // 2
    core = tp_index % 2
    even = seq_index % 2 == 0

    input_values = input_rows.astype(jnp.float32)
    inverse_norm = lax.rsqrt(
        jnp.mean(input_values * input_values, axis=-1, keepdims=True) + epsilon
    )
    gain_values = norm_gain[0].astype(jnp.float32)
    normed = (input_values * inverse_norm * gain_values).astype(jnp.bfloat16)
    cosine, sine = rotary_tables(total_rows)

    def source_of(steps):
        return (seq_index + seq_count - steps) % seq_count

    def target_of(steps):
        return (seq_index + steps) % seq_count

    def spread(value):
        mine = lax.dynamic_slice_in_dim(value, core * half_rows, half_rows, 0)
        own = jnp.zeros((seq_count, half_rows, local_width), value.dtype)
        for steps in range(seq_count):
            piece = columns(mine, target_of(steps) * local_width, local_width)
            if steps:
                piece = turn(piece, "seq", steps)
            own = lax.dynamic_update_slice(own, piece[None], (source_of(steps), 0, 0))
        other = swap(own, "tp", 1)
        low = jnp.where(core == 0, own, other)
        high = jnp.where(core == 0, other, own)
        return jnp.stack([low, high], axis=1).reshape(total_rows, local_width)

    normed_spread = spread(normed)
    upstream_spread = spread(upstream_rows)

    paired = jnp.stack(
        [
            key_block.reshape(local_width, local_groups, HEAD_DIM),
            value_block.reshape(local_width, local_groups, HEAD_DIM),
        ],
        axis=2,
    ).reshape(local_width, local_heads * HEAD_DIM)
    input_weights = []
    output_weights = []
    for steps in range(seq_count):
        first = target_of(steps) * HEAD_DIM
        input_weights.append(
            jnp.concatenate(
                [columns(query_block, first, HEAD_DIM), columns(paired, first, HEAD_DIM)], axis=1
            )
        )
        output_weights.append(columns(output_block, first, HEAD_DIM))

    def summed(left, weights):
        total = jnp.dot(left, weights[0], preferred_element_type=jnp.float32)
        for steps in range(1, seq_count):
            part = jnp.dot(left, weights[steps], preferred_element_type=jnp.float32)
            total = total + turn(part.astype(jnp.bfloat16), "seq", steps).astype(jnp.float32)
        return total

    projected = summed(normed_spread, input_weights)
    delta = summed(upstream_spread, output_weights).astype(jnp.bfloat16)

    def rotated(values):
        return values * cosine + half_swapped(values) * sine

    query = rotated(projected[:, :HEAD_DIM]).astype(jnp.bfloat16)
    pair_mine = projected[:, HEAD_DIM:]
    pair_mine = jnp.where(even, rotated(pair_mine), pair_mine).astype(jnp.bfloat16)
    pair_other = swap(pair_mine, "seq", 1)
    key = jnp.where(even, pair_mine, pair_other)
    value = jnp.where(even, pair_other, pair_mine)
    query_delta, attended, key_part, value_part = attend(query, key, value, delta, cosine, sine)
    pair_sent = swap(jnp.where(even, value_part, key_part), "seq", 1)
    pair_kept = jnp.where(even, key_part, value_part)
    pair_delta = (pair_kept.astype(jnp.float32) + pair_sent.astype(jnp.float32)).astype(
        jnp.bfloat16
    )
    attended_all = gathered_line(attended, "seq")
    deltas_all = gathered_line(jnp.concatenate([query_delta, pair_delta], axis=1), "seq")

    normed_partial = contract_last(
        jnp.concatenate(deltas_all, axis=1), jnp.concatenate(input_weights, axis=1)
    ).reshape(seq_count, tp_count // 2, 2, block_rows // tp_count, local_width)
    kept = columns_at(normed_partial, core, 2)
    sent = columns_at(normed_partial, 1 - core, 2).astype(jnp.bfloat16)
    reduced = kept + swap(sent, "tp", 1).astype(jnp.float32)
    piece_rows = block_rows // tp_count
    tile = tp_index // 2
    kept = columns_at(reduced, tile, 1)
    for other in range(1, tp_count // 2):
        sent = columns_at(reduced, tile ^ other, 1).astype(jnp.bfloat16)
        kept = kept + swap(sent, "tp", 2 * other).astype(jnp.float32)
    reduced = kept.astype(jnp.bfloat16)
    normed_delta = jnp.zeros((piece_rows, model_width), jnp.bfloat16)
    for steps in range(seq_count):
        piece = lax.dynamic_index_in_dim(reduced, target_of(steps), 0, keepdims=False)
        if steps:
            piece = turn(piece, "seq", steps)
        normed_delta = lax.dynamic_update_slice(
            normed_delta, piece, (0, source_of(steps) * local_width)
        )
    normed_delta = normed_delta.astype(jnp.float32)
    first_row = tp_index * piece_rows
    input_piece = lax.dynamic_slice_in_dim(input_rows, first_row, piece_rows, 0).astype(jnp.float32)
    upstream_piece = lax.dynamic_slice_in_dim(upstream_rows, first_row, piece_rows, 0)
    norm_piece = lax.dynamic_slice_in_dim(inverse_norm, first_row, piece_rows, 0)
    row_dot = jnp.sum(gain_values * normed_delta * input_piece, axis=-1, keepdims=True)
    input_delta = (
        upstream_piece.astype(jnp.float32)
        + norm_piece * gain_values * normed_delta
        - input_piece * (norm_piece * norm_piece * norm_piece) * row_dot / model_width
    ).astype(jnp.bfloat16)
    passed = shifted_2(input_delta, "section", -1)[None]
    bit = 1
    while bit < tp_count:
        other = swap(passed, "tp", bit)
        low = (tp_index // bit) % 2 == 0
        passed = jnp.concatenate(
            [jnp.where(low, passed, other), jnp.where(low, other, passed)], axis=0
        )
        bit *= 2
    passed = passed.reshape(block_rows, model_width)

    gain_part = jnp.sum(normed_delta * input_piece * norm_piece, axis=0).reshape(tp_count, -1)
    gain_sum = lax.dynamic_index_in_dim(gain_part, tp_index, 0, keepdims=True)
    for other in range(1, tp_count):
        sent = lax.dynamic_index_in_dim(gain_part, tp_index ^ other, 0, keepdims=True)
        gain_sum = gain_sum + swap(sent, "tp", other)
    gain_total = gain_sum
    for steps in range(1, seq_count):
        gain_total = gain_total + turn(gain_sum, "seq", steps)

    query_grad = jnp.zeros(query_block.shape, jnp.bfloat16)
    pair_grad = jnp.zeros(query_block.shape, jnp.bfloat16)
    output_grad = jnp.zeros(output_block.shape, jnp.bfloat16)
    for steps in range(seq_count):
        first = target_of(steps) * HEAD_DIM
        grad = contract_rows(normed_spread, deltas_all[steps]).astype(jnp.bfloat16)
        query_grad = lax.dynamic_update_slice(query_grad, grad[:, :HEAD_DIM], (0, first))
        pair_grad = lax.dynamic_update_slice(pair_grad, grad[:, HEAD_DIM:], (0, first))
        grad = contract_rows(upstream_spread, attended_all[steps]).astype(jnp.bfloat16)
        output_grad = lax.dynamic_update_slice(output_grad, grad, (0, first))
    pair_grad = pair_grad.reshape(local_width, local_groups, 2, HEAD_DIM)
    key_grad = pair_grad[:, :, 0].reshape(key_block.shape)
    value_grad = pair_grad[:, :, 1].reshape(value_block.shape)
    return (
        passed[None],
        query_grad[None],
        key_grad[None],
        value_grad[None],
        output_grad[None],
        gain_total.reshape(1, -1),
    )


def columns_at(value, index, axis):
    return lax.dynamic_index_in_dim(value, index, axis, keepdims=False)


def per_device(
    layer_input, upstream, norm_gain, query_weight, key_weight, value_weight, output_weight
):
    seq_count = lax.axis_size("seq")
    tp_count = lax.axis_size("tp")
    block_rows = layer_input.shape[1]
    local_heads = query_weight.shape[2] // HEAD_DIM
    local_groups = key_weight.shape[2] // HEAD_DIM
    by_head = (
        local_heads == seq_count
        and local_heads == 2 * local_groups
        and tp_count & (tp_count - 1) == 0
        and tp_count > 1
        and block_rows % (8 * tp_count) == 0
        and seq_count * block_rows <= min(WINDOW, 1024)
    )
    run = per_device_heads if by_head else per_device_rows
    return run(
        layer_input, upstream, norm_gain, query_weight, key_weight, value_weight, output_weight
    )


def solution(mesh):
    in_specs = (
        P("section", "seq", None),
        P("section", "seq", None),
        P("section", None),
        P("section", "seq", "tp"),
        P("section", "seq", "tp"),
        P("section", "seq", "tp"),
        P("section", "seq", "tp"),
    )
    out_specs = (
        P("section", "seq", None),
        P("section", "seq", "tp"),
        P("section", "seq", "tp"),
        P("section", "seq", "tp"),
        P("section", "seq", "tp"),
        P("section", "tp"),
    )
    return jax.shard_map(
        per_device, mesh=mesh, in_specs=in_specs, out_specs=out_specs, check_vma=False
    )
```
